8 devices in a mesh: ep: 8 (over z, y, x, core).
Axes of the slice: x: 2, y: 2, z: 1, core: 2. Of those that a mesh axis runs over, the one named last changes fastest.
Arguments:
- x_in: bfloat16 [4096, 3584], P('ep')
- route_idx: int32 [4096, 8], P('ep')
- gate_w: bfloat16 [4096, 8], P('ep')
- dy_in: bfloat16 [4096, 3584], P('ep')
- w_gate: bfloat16 [8, 3584, 2560], P('ep')
- w_up: bfloat16 [8, 3584, 2560], P('ep')
- w_down: bfloat16 [8, 2560, 3584], P('ep')
- hot_gate: bfloat16 [3584, 2560], replicated
- hot_up: bfloat16 [3584, 2560], replicated
- hot_down: bfloat16 [2560, 3584], replicated
Outputs:
- output 1: bfloat16 [4096, 3584], P('ep')
- output 2: bfloat16 [4096, 3584], P('ep')
- output 3: float32 [8, 3584, 2560], P('ep')
- output 4: float32 [8, 3584, 2560], P('ep')
- output 5: float32 [8, 2560, 3584], P('ep')
- output 6: float32 [3584, 2560], P(None, 'ep')
- output 7: float32 [3584, 2560], P(None, 'ep')
- output 8: float32 [2560, 3584], P('ep')
All inputs are finite; a program needn't handle non-finite values.
Results may differ from the reference program's by a relative error of at most 0.0018.
Values are sent between devices in bfloat16 or wider.
A program may use at most 1 GiB of HBM per device.

```python
import jax
import jax.numpy as jnp
from jax import lax

N_DEV = 8
TOK_DEV = 512
D_MODEL = 3584
D_FF = 2560
TOP_K = 8

SLOT_CAP = min(TOK_DEV, 2 * TOK_DEV * TOP_K // N_DEV)
HOT_CAP = 3 * TOK_DEV // 4
TOTAL = N_DEV * TOK_DEV


def draw_routes(rng_key):
    heavy_key, weight_key, hot_key, pick_key, order_key, shift_key = jax.random.split(rng_key, 6)
    expert_ids = jnp.arange(N_DEV, dtype=jnp.int32)
    heavy = jax.random.randint(heavy_key, (N_DEV,), 0, N_DEV)
    is_heavy = expert_ids[None, :] == heavy[:, None]
    weight = jnp.where(is_heavy, 0, jax.random.randint(weight_key, (N_DEV, N_DEV), 1, 9))
    hot_count = jax.random.randint(hot_key, (N_DEV,), HOT_CAP // 4, HOT_CAP + 1)
    hot_count = jnp.where(expert_ids == jax.random.randint(pick_key, (), 0, N_DEV), HOT_CAP, hot_count)
    rest = TOK_DEV * TOP_K - hot_count - SLOT_CAP
    base = jnp.minimum((rest[:, None] * weight) // jnp.sum(weight, axis=1, keepdims=True), SLOT_CAP)
    room = jnp.where(is_heavy, 0, SLOT_CAP - base)
    deficit = rest - jnp.sum(base, axis=1)
    before = jnp.cumsum(room, axis=1) - room
    extra = jnp.minimum(jnp.maximum(deficit[:, None] - before, 0), room)
    load = base + extra + jnp.where(is_heavy, SLOT_CAP, 0)
    bounds = jnp.cumsum(jnp.concatenate([load, hot_count[:, None]], axis=1), axis=1)
    positions = jnp.arange(TOK_DEV * TOP_K, dtype=jnp.int32)
    ordered = jax.vmap(lambda bound_row: jnp.searchsorted(bound_row, positions, side='right'))(bounds)
    grid = ordered.reshape(N_DEV, TOP_K, TOK_DEV).transpose(0, 2, 1)
    token_order = jax.vmap(lambda sub_key: jax.random.permutation(sub_key, TOK_DEV))(jax.random.split(order_key, N_DEV))
    grid = jnp.take_along_axis(grid, token_order[:, :, None], axis=1)
    shift = jax.random.randint(shift_key, (N_DEV, TOK_DEV, 1), 0, TOP_K)
    col_index = (jnp.arange(TOP_K, dtype=jnp.int32)[None, None, :] + shift) % TOP_K
    grid = jnp.take_along_axis(grid, col_index, axis=2)
    return grid.reshape(TOTAL, TOP_K).astype(jnp.int32)


def setup_inputs(seed: int = 0) -> dict:
    sub_keys = jax.random.split(jax.random.key(seed), 10)
    in_scale = D_MODEL ** -0.5
    hid_scale = D_FF ** -0.5
    x_in = jax.random.normal(sub_keys[0], (TOTAL, D_MODEL), jnp.float32).astype(jnp.bfloat16)
    route_idx = draw_routes(sub_keys[1])
    gate_w = jax.random.uniform(sub_keys[2], (TOTAL, TOP_K), jnp.float32, 0.5, 1.5).astype(jnp.bfloat16)
    dy_in = jax.random.normal(sub_keys[3], (TOTAL, D_MODEL), jnp.float32).astype(jnp.bfloat16)
    w_gate = (jax.random.normal(sub_keys[4], (N_DEV, D_MODEL, D_FF), jnp.float32) * in_scale).astype(jnp.bfloat16)
    w_up = (jax.random.normal(sub_keys[5], (N_DEV, D_MODEL, D_FF), jnp.float32) * in_scale).astype(jnp.bfloat16)
    w_down = (jax.random.normal(sub_keys[6], (N_DEV, D_FF, D_MODEL), jnp.float32) * hid_scale).astype(jnp.bfloat16)
    hot_gate = (jax.random.normal(sub_keys[7], (D_MODEL, D_FF), jnp.float32) * in_scale).astype(jnp.bfloat16)
    hot_up = (jax.random.normal(sub_keys[8], (D_MODEL, D_FF), jnp.float32) * in_scale).astype(jnp.bfloat16)
    hot_down = (jax.random.normal(sub_keys[9], (D_FF, D_MODEL), jnp.float32) * hid_scale).astype(jnp.bfloat16)
    return {'x_in': x_in, 'route_idx': route_idx, 'gate_w': gate_w, 'dy_in': dy_in, 'w_gate': w_gate, 'w_up': w_up, 'w_down': w_down, 'hot_gate': hot_gate, 'hot_up': hot_up, 'hot_down': hot_down}


def silu_parts(pre_gate):
    sig_val = jax.nn.sigmoid(pre_gate)
    return pre_gate * sig_val, sig_val * (1.0 + pre_gate * (1.0 - sig_val))


def expert_pass(x_rows, d_rows, gate_mat, up_mat, down_mat):
    u_val = jnp.dot(x_rows, gate_mat, preferred_element_type=jnp.float32)
    v_val = jnp.dot(x_rows, up_mat, preferred_element_type=jnp.float32)
    silu_val, silu_grad = silu_parts(u_val)
    hidden = (silu_val * v_val).astype(jnp.bfloat16)
    result = jnp.dot(hidden, down_mat, preferred_element_type=jnp.float32).astype(jnp.bfloat16)
    grad_hidden = jnp.dot(d_rows, down_mat.T, preferred_element_type=jnp.float32).astype(jnp.bfloat16).astype(jnp.float32)
    grad_u = (grad_hidden * v_val * silu_grad).astype(jnp.bfloat16)
    grad_v = (grad_hidden * silu_val).astype(jnp.bfloat16)
    grad_x = (jnp.dot(grad_u, gate_mat.T, preferred_element_type=jnp.float32) + jnp.dot(grad_v, up_mat.T, preferred_element_type=jnp.float32)).astype(jnp.bfloat16)
    grad_gate = jnp.dot(x_rows.T, grad_u, preferred_element_type=jnp.float32)
    grad_up = jnp.dot(x_rows.T, grad_v, preferred_element_type=jnp.float32)
    grad_down = jnp.dot(hidden.T, d_rows, preferred_element_type=jnp.float32)
    return result, grad_x, (grad_gate, grad_up, grad_down)


def reference(x_in, route_idx, gate_w, dy_in, w_gate, w_up, w_down, hot_gate, hot_up, hot_down):
    flat_ids = route_idx.reshape(-1)
    n_assign = flat_ids.shape[0]
    order = jnp.argsort(flat_ids, stable=True)
    starts = jnp.searchsorted(flat_ids[order], jnp.arange(N_DEV + 2, dtype=jnp.int32), side='left')
    gate_flat = gate_w.reshape(-1)

    def take_block(first, last, max_rows):
        position = first + jnp.arange(max_rows, dtype=jnp.int32)
        assign = jnp.where(position < last, order[jnp.minimum(position, n_assign - 1)], n_assign)
        token = assign // TOP_K
        x_rows = jnp.take(x_in, token, axis=0, mode='fill', fill_value=0)
        gate_rows = jnp.take(gate_flat, assign, mode='fill', fill_value=0).astype(jnp.float32)
        dy_rows = jnp.take(dy_in, token, axis=0, mode='fill', fill_value=0).astype(jnp.float32)
        d_rows = (gate_rows[:, None] * dy_rows).astype(jnp.bfloat16)
        return token, gate_rows, x_rows, d_rows

    def add_block(sums, token, gate_rows, result, grad_x):
        y_sum, dx_sum = sums
        y_sum = y_sum.at[token].add(gate_rows[:, None] * result.astype(jnp.float32), mode='drop')
        dx_sum = dx_sum.at[token].add(grad_x.astype(jnp.float32), mode='drop')
        return y_sum, dx_sum

    def regular_step(sums, expert_args):
        gate_mat, up_mat, down_mat, first, last = expert_args
        token, gate_rows, x_rows, d_rows = take_block(first, last, N_DEV * SLOT_CAP)
        result, grad_x, grads = expert_pass(x_rows, d_rows, gate_mat, up_mat, down_mat)
        return add_block(sums, token, gate_rows, result, grad_x), grads

    zero_sum = jnp.zeros((TOTAL, D_MODEL), jnp.float32)
    sums, (dw_gate, dw_up, dw_down) = lax.scan(regular_step, (zero_sum, zero_sum), (w_gate, w_up, w_down, starts[:N_DEV], starts[1:N_DEV + 1]))
    token, gate_rows, x_rows, d_rows = take_block(starts[N_DEV], starts[N_DEV + 1], N_DEV * HOT_CAP)
    result, grad_x, (dhot_gate, dhot_up, dhot_down) = expert_pass(x_rows, d_rows, hot_gate, hot_up, hot_down)
    y_sum, dx_sum = add_block(sums, token, gate_rows, result, grad_x)
    return (y_sum.astype(jnp.bfloat16), dx_sum.astype(jnp.bfloat16), dw_gate, dw_up, dw_down, dhot_gate, dhot_up, dhot_down)
```

```python
import jax
import jax.numpy as jnp
from jax import lax
from jax.sharding import PartitionSpec as P

F32 = jnp.float32
BF16 = jnp.bfloat16
CONTRACT_LAST = (((1,), (1,)), ((), ()))
CONTRACT_FIRST = (((0,), (0,)), ((), ()))


def mm(a, b):
    return jnp.dot(a, b, preferred_element_type=F32)


def mm_last(a, b):
    return lax.dot_general(a, b, CONTRACT_LAST, preferred_element_type=F32)


def mm_first(a, b):
    return lax.dot_general(a, b, CONTRACT_FIRST, preferred_element_type=F32)


def rounded(value):
    return lax.reduce_precision(value, exponent_bits=8, mantissa_bits=7)


def silu_parts(pre_gate):
    sig_val = jax.nn.sigmoid(pre_gate)
    return pre_gate * sig_val, sig_val * (1.0 + pre_gate * (1.0 - sig_val))


def dense_gates(route_loc, gate_loc, n_choice):
    hit = route_loc[:, :, None] == jnp.arange(n_choice, dtype=jnp.int32)[None, None, :]
    gates = jnp.sum(jnp.where(hit, gate_loc.astype(F32)[:, :, None], 0.0), axis=1)
    return gates, jnp.any(hit, axis=1)


def hidden_of(u_val, v_val, keep):
    silu_val, _ = silu_parts(u_val)
    return jnp.where(keep, silu_val * v_val, 0.0).astype(BF16)


def hidden_grads(u_val, v_val, grad_hidden, keep):
    silu_val, silu_grad = silu_parts(u_val)
    p_val = rounded(grad_hidden)
    du = jnp.where(keep, p_val * v_val * silu_grad, 0.0).astype(BF16)
    dv = jnp.where(keep, p_val * silu_val, 0.0).astype(BF16)
    return du, dv


def solution(mesh):
    n_dev = mesh.shape['ep']

    def local_step(x_loc, route_loc, gate_loc, dy_loc, w_gate, w_up, w_down, hot_gate, hot_up, hot_down):
        me = lax.axis_index('ep')
        tok, d_model = x_loc.shape
        d_ff = hot_gate.shape[1]
        part = d_ff // n_dev
        w_gate, w_up, w_down = w_gate[0], w_up[0], w_down[0]

        gates, chosen = dense_gates(route_loc, gate_loc, n_dev + 1)
        table = jnp.concatenate([gates, chosen.astype(F32)], axis=1)
        table_all = lax.all_gather(table, 'ep', axis=0, tiled=True)
        gates_all, chosen_all = table_all[:, :n_dev + 1], table_all[:, n_dev + 1:]
        mine = (jnp.arange(n_dev + 1, dtype=jnp.int32) == me)[None, :]
        g_mine = jnp.sum(jnp.where(mine, gates_all, 0.0), axis=1, keepdims=True)
        keep_mine = jnp.sum(jnp.where(mine, chosen_all, 0.0), axis=1, keepdims=True) > 0.5
        g_hot, keep_hot = gates_all[:, n_dev:], chosen_all[:, n_dev:] > 0.5
        g_hot_loc, keep_hot_loc = gates[:, n_dev:], chosen[:, n_dev:]

        x_all = lax.all_gather(x_loc, 'ep', axis=0, tiled=True)
        dy_all = lax.all_gather(dy_loc, 'ep', axis=0, tiled=True)

        uh = mm(x_loc, hot_gate)
        vh = mm(x_loc, hot_up)
        oh = mm(hidden_of(uh, vh, keep_hot_loc), hot_down)
        y_hot = g_hot_loc * rounded(oh)
        qh = (g_hot_loc * dy_loc.astype(F32)).astype(BF16)
        duh, dvh = hidden_grads(uh, vh, mm_last(qh, hot_down), keep_hot_loc)
        dx_hot = rounded(mm_last(duh, hot_gate) + mm_last(dvh, hot_up))

        x_all, y_hot, dx_hot = lax.optimization_barrier((x_all, y_hot, dx_hot))

        u_val = mm(x_all, w_gate)
        v_val = mm(x_all, w_up)
        hidden = hidden_of(u_val, v_val, keep_mine)
        out = g_mine * rounded(mm(hidden, w_down))
        y_sum = lax.psum_scatter(out, 'ep', scatter_dimension=0, tiled=True)
        q_mine = (g_mine * dy_all.astype(F32)).astype(BF16)
        du, dv = hidden_grads(u_val, v_val, mm_last(q_mine, w_down), keep_mine)
        r_val = rounded(mm_last(du, w_gate) + mm_last(dv, w_up))
        dx_sum = lax.psum_scatter(r_val, 'ep', scatter_dimension=0, tiled=True)
        grad_gate = mm_first(x_all, du)
        grad_up = mm_first(x_all, dv)
        grad_down = mm_first(hidden, q_mine)

        hg = lax.dynamic_slice_in_dim(hot_gate, me * part, part, axis=1)
        hu = lax.dynamic_slice_in_dim(hot_up, me * part, part, axis=1)
        hd = lax.dynamic_slice_in_dim(hot_down, me * part, part, axis=0)
        uv = mm(x_all, jnp.concatenate([hg, hu], axis=1))
        us, vs = uv[:, :part], uv[:, part:]
        q_hot = (g_hot * dy_all.astype(F32)).astype(BF16)
        dus, dvs = hidden_grads(us, vs, mm_last(q_hot, hd), keep_hot)
        hot_duv = mm_first(x_all, jnp.concatenate([dus, dvs], axis=1))
        hot_ddown = mm_first(hidden_of(us, vs, keep_hot), q_hot)

        y_loc = (y_sum + y_hot).astype(BF16)
        dx_loc = (dx_sum + dx_hot).astype(BF16)
        return (y_loc, dx_loc, grad_gate[None], grad_up[None], grad_down[None], hot_duv[:, :part], hot_duv[:, part:], hot_ddown)

    row_spec = P('ep', None)
    expert_spec = P('ep', None, None)
    whole_spec = P(None, None)
    return jax.shard_map(local_step, mesh=mesh, in_specs=(row_spec, row_spec, row_spec, row_spec, expert_spec, expert_spec, expert_spec, whole_spec, whole_spec, whole_spec), out_specs=(row_spec, row_spec, expert_spec, expert_spec, expert_spec, P(None, 'ep'), P(None, 'ep'), P('ep', None)), check_vma=False)
```

```python
import jax
import jax.numpy as jnp
from jax import lax
from jax.sharding import PartitionSpec as P

F32 = jnp.float32
BF16 = jnp.bfloat16
CONTRACT_LAST = (((1,), (1,)), ((), ()))
CONTRACT_FIRST = (((0,), (0,)), ((), ()))


def mm(a, b):
    return jnp.dot(a, b, preferred_element_type=F32)


def mm_last(a, b):
    return lax.dot_general(a, b, CONTRACT_LAST, preferred_element_type=F32)


def mm_first(a, b):
    return lax.dot_general(a, b, CONTRACT_FIRST, preferred_element_type=F32)


def rounded(value):
    return lax.reduce_precision(value, exponent_bits=8, mantissa_bits=7)


def silu_parts(pre_gate):
    sig_val = jax.nn.sigmoid(pre_gate)
    return pre_gate * sig_val, sig_val * (1.0 + pre_gate * (1.0 - sig_val))


def dense_gates(route_loc, gate_loc, n_choice):
    hit = route_loc[:, :, None] == jnp.arange(n_choice, dtype=jnp.int32)[None, None, :]
    gates = jnp.sum(jnp.where(hit, gate_loc.astype(F32)[:, :, None], 0.0), axis=1)
    return gates, jnp.any(hit, axis=1)


def hidden_of(u_val, v_val, keep):
    silu_val, _ = silu_parts(u_val)
    return jnp.where(keep, silu_val * v_val, 0.0).astype(BF16)


def hidden_grads(u_val, v_val, grad_hidden, keep):
    silu_val, silu_grad = silu_parts(u_val)
    p_val = rounded(grad_hidden)
    du = jnp.where(keep, p_val * v_val * silu_grad, 0.0).astype(BF16)
    dv = jnp.where(keep, p_val * silu_val, 0.0).astype(BF16)
    return du, dv


def solution(mesh):
    n_dev = mesh.shape['ep']

    def local_step(x_loc, route_loc, gate_loc, dy_loc, w_gate, w_up, w_down, hot_gate, hot_up, hot_down):
        me = lax.axis_index('ep')
        tok, d_model = x_loc.shape
        d_ff = hot_gate.shape[1]
        part = d_ff // n_dev
        w_gate, w_up, w_down = w_gate[0], w_up[0], w_down[0]

        gates, chosen = dense_gates(route_loc, gate_loc, n_dev + 1)
        table = jnp.concatenate([gates, chosen.astype(F32)], axis=1)
        table_all = lax.all_gather(table, 'ep', axis=0, tiled=True)
        gates_all, chosen_all = table_all[:, :n_dev + 1], table_all[:, n_dev + 1:]
        mine = (jnp.arange(n_dev + 1, dtype=jnp.int32) == me)[None, :]
        g_mine = jnp.sum(jnp.where(mine, gates_all, 0.0), axis=1, keepdims=True)
        keep_mine = jnp.sum(jnp.where(mine, chosen_all, 0.0), axis=1, keepdims=True) > 0.5
        g_hot, keep_hot = gates_all[:, n_dev:], chosen_all[:, n_dev:] > 0.5
        g_hot_loc, keep_hot_loc = gates[:, n_dev:], chosen[:, n_dev:]

        x_all = lax.all_gather(x_loc, 'ep', axis=0, tiled=True)
        dy_all = lax.all_gather(dy_loc, 'ep', axis=0, tiled=True)

        uh = mm(x_loc, hot_gate)
        vh = mm(x_loc, hot_up)
        oh = mm(hidden_of(uh, vh, keep_hot_loc), hot_down)
        y_hot = g_hot_loc * rounded(oh)
        qh = (g_hot_loc * dy_loc.astype(F32)).astype(BF16)
        duh, dvh = hidden_grads(uh, vh, mm_last(qh, hot_down), keep_hot_loc)
        dx_hot = rounded(mm_last(duh, hot_gate) + mm_last(dvh, hot_up))

        x_all, y_hot, dx_hot = lax.optimization_barrier((x_all, y_hot, dx_hot))

        u_val = mm(x_all, w_gate)
        v_val = mm(x_all, w_up)
        hidden = hidden_of(u_val, v_val, keep_mine)
        u_val, v_val, hidden = lax.optimization_barrier((u_val, v_val, hidden))
        out = g_mine * rounded(mm(hidden, w_down))
        out, dy_all = lax.optimization_barrier((out, dy_all))
        y_sum = lax.psum_scatter(out, 'ep', scatter_dimension=0, tiled=True)
        q_mine = (g_mine * dy_all.astype(F32)).astype(BF16)
        du, dv = hidden_grads(u_val, v_val, mm_last(q_mine, w_down), keep_mine)
        r_val = rounded(mm_last(du, w_gate) + mm_last(dv, w_up))
        dx_sum = lax.psum_scatter(r_val, 'ep', scatter_dimension=0, tiled=True)
        grad_gate = mm_first(x_all, du)
        grad_up = mm_first(x_all, dv)
        grad_down = mm_first(hidden, q_mine)

        hg = lax.dynamic_slice_in_dim(hot_gate, me * part, part, axis=1)
        hu = lax.dynamic_slice_in_dim(hot_up, me * part, part, axis=1)
        hd = lax.dynamic_slice_in_dim(hot_down, me * part, part, axis=0)
        uv = mm(x_all, jnp.concatenate([hg, hu], axis=1))
        us, vs = uv[:, :part], uv[:, part:]
        q_hot = (g_hot * dy_all.astype(F32)).astype(BF16)
        dus, dvs = hidden_grads(us, vs, mm_last(q_hot, hd), keep_hot)
        hot_duv = mm_first(x_all, jnp.concatenate([dus, dvs], axis=1))
        hot_ddown = mm_first(hidden_of(us, vs, keep_hot), q_hot)

        y_loc = (y_sum + y_hot).astype(BF16)
        dx_loc = (dx_sum + dx_hot).astype(BF16)
        return (y_loc, dx_loc, grad_gate[None], grad_up[None], grad_down[None], hot_duv[:, :part], hot_duv[:, part:], hot_ddown)

    row_spec = P('ep', None)
    expert_spec = P('ep', None, None)
    whole_spec = P(None, None)
    return jax.shard_map(local_step, mesh=mesh, in_specs=(row_spec, row_spec, row_spec, row_spec, expert_spec, expert_spec, expert_spec, whole_spec, whole_spec, whole_spec), out_specs=(row_spec, row_spec, expert_spec, expert_spec, expert_spec, P(None, 'ep'), P(None, 'ep'), P('ep', None)), check_vma=False)
```
